32 devices in a mesh: dp: 1 (over z), tp: 4 (over y), sp: 8 (over x, core).
Axes of the slice: x: 4, y: 4, z: 1, core: 2. Of those that a mesh axis runs over, the one named last changes fastest.
The devices are a block of a 4x4x8 slice.
Arguments:
- hidden: bfloat16 [256, 4096], P('dp')
- norm_w: bfloat16 [4096], replicated
- w_q: bfloat16 [4096, 12288], P(None, 'tp')
- b_q: bfloat16 [12288], P('tp')
- w_k: bfloat16 [4096, 1024], P(None, 'tp')
- b_k: bfloat16 [1024], P('tp')
- w_v: bfloat16 [4096, 1024], P(None, 'tp')
- b_v: bfloat16 [1024], P('tp')
- w_o: bfloat16 [12288, 4096], P('tp')
- k_cache: bfloat16 [256, 1024, 8, 128], P('dp', 'sp', 'tp')
- v_cache: bfloat16 [256, 1024, 8, 128], P('dp', 'sp', 'tp')
- positions: int32 [256], P('dp')
- seq_lens: int32 [256], P('dp')
Outputs:
- output 1: bfloat16 [256, 4096], P('dp')
- output 2: bfloat16 [256, 8, 128], P('dp', 'tp')
- output 3: bfloat16 [256, 8, 128], P('dp', 'tp')
All inputs are finite; a program needn't handle non-finite values.
Results may differ from the reference program's by a relative error of at most 0.00743964.
Values sent between devices are 32-bit elements.
A program may use at most 768 MiB of HBM per device.

```python
import jax
import jax.numpy as jnp
from jax import lax

BATCH = 256
SEQ_LEN = 1024
D_MODEL = 4096
N_HEADS = 96
KV_GROUPS = 8
HEAD_DIM = 128
ROT_DIM = HEAD_DIM // 2
PER_GROUP = N_HEADS // KV_GROUPS
Q_COLS = N_HEADS * HEAD_DIM
KV_COLS = KV_GROUPS * HEAD_DIM
RMS_EPS = 1.5625e-7
ROPE_BASE = 10000.0


def normal_draw(key, shape, std):
    return std * jax.random.normal(key, shape, jnp.float32)


def setup_inputs(seed: int = 0, part: int = 0) -> dict:
    shared_keys = jax.random.split(jax.random.key(seed), 8)
    part_keys = jax.random.split(jax.random.fold_in(jax.random.key(seed + 1), part), 5)
    val_scale = (SEQ_LEN ** 0.5) / 4.0
    cache_shape = (BATCH, SEQ_LEN, KV_GROUPS, HEAD_DIM)
    seq_lens = jax.random.randint(part_keys[3], (BATCH,), SEQ_LEN // 8, SEQ_LEN + 1, dtype=jnp.int32)
    seq_lens = seq_lens.at[0].set(SEQ_LEN).at[1].set(SEQ_LEN // 8)
    positions = seq_lens + jax.random.randint(part_keys[4], (BATCH,), 0, SEQ_LEN + 1, dtype=jnp.int32)
    return {
        'hidden': normal_draw(part_keys[0], (BATCH, D_MODEL), 1.0).astype(jnp.bfloat16),
        'norm_w': (1.0 + normal_draw(shared_keys[0], (D_MODEL,), 0.3)).astype(jnp.bfloat16),
        'w_q': normal_draw(shared_keys[1], (D_MODEL, Q_COLS), D_MODEL ** -0.5).astype(jnp.bfloat16),
        'b_q': normal_draw(shared_keys[2], (Q_COLS,), 0.5).astype(jnp.bfloat16),
        'w_k': normal_draw(shared_keys[3], (D_MODEL, KV_COLS), D_MODEL ** -0.5).astype(jnp.bfloat16),
        'b_k': normal_draw(shared_keys[4], (KV_COLS,), 0.5).astype(jnp.bfloat16),
        'w_v': normal_draw(shared_keys[5], (D_MODEL, KV_COLS), D_MODEL ** -0.5).astype(jnp.bfloat16),
        'b_v': normal_draw(shared_keys[6], (KV_COLS,), 0.5).astype(jnp.bfloat16),
        'w_o': normal_draw(shared_keys[7], (Q_COLS, D_MODEL), Q_COLS ** -0.5).astype(jnp.bfloat16),
        'k_cache': normal_draw(part_keys[1], cache_shape, 1.4).astype(jnp.bfloat16),
        'v_cache': normal_draw(part_keys[2], cache_shape, val_scale).astype(jnp.bfloat16),
        'positions': positions,
        'seq_lens': seq_lens,
    }


def apply_rotary(heads_in, positions):
    half_rot = ROT_DIM // 2
    inv_freq = ROPE_BASE ** (-2.0 * jnp.arange(half_rot, dtype=jnp.float32) / ROT_DIM)
    angles = positions.astype(jnp.float32)[:, None, None] * inv_freq
    cos_t = jnp.cos(angles)
    sin_t = jnp.sin(angles)
    rot_pairs = heads_in[..., :ROT_DIM].astype(jnp.float32).reshape(heads_in.shape[:-1] + (half_rot, 2))
    even_part = rot_pairs[..., 0]
    odd_part = rot_pairs[..., 1]
    rotated = jnp.stack([even_part * cos_t - odd_part * sin_t, even_part * sin_t + odd_part * cos_t], axis=-1)
    rotated = rotated.reshape(heads_in.shape[:-1] + (ROT_DIM,)).astype(jnp.bfloat16)
    return jnp.concatenate([rotated, heads_in[..., ROT_DIM:]], axis=-1)


def project(normed, weight, bias_vec):
    return (jnp.dot(normed, weight, preferred_element_type=jnp.float32) + bias_vec.astype(jnp.float32)).astype(jnp.bfloat16)


def reference(hidden, norm_w, w_q, b_q, w_k, b_k, w_v, b_v, w_o, k_cache, v_cache, positions, seq_lens):
    x_f32 = hidden.astype(jnp.float32)
    mean_sq = jnp.mean(x_f32 * x_f32, axis=-1, keepdims=True)
    normed = (x_f32 * lax.rsqrt(mean_sq + RMS_EPS) * norm_w.astype(jnp.float32)).astype(jnp.bfloat16)
    q_rot = apply_rotary(project(normed, w_q, b_q).reshape(BATCH, N_HEADS, HEAD_DIM), positions)
    k_rot = apply_rotary(project(normed, w_k, b_k).reshape(BATCH, KV_GROUPS, HEAD_DIM), positions)
    v_new = project(normed, w_v, b_v).reshape(BATCH, KV_GROUPS, HEAD_DIM)
    attn_scale = HEAD_DIM ** -0.5
    cache_idx = jnp.arange(SEQ_LEN)

    def one_row(row_args):
        q_row, k_row, v_row, k_tok, v_tok, length = row_args
        q_grp = q_row.reshape(KV_GROUPS, PER_GROUP, HEAD_DIM).astype(jnp.float32)
        s_cache = jnp.einsum('gqd,sgd->gqs', q_grp, k_row.astype(jnp.float32)) * attn_scale
        s_cache = jnp.where((cache_idx < length)[None, None, :], s_cache, -jnp.inf)
        s_new = jnp.einsum('gqd,gd->gq', q_grp, k_tok.astype(jnp.float32)) * attn_scale
        m_top = jnp.maximum(jnp.max(s_cache, axis=-1), s_new)
        p_cache = jnp.exp(s_cache - m_top[..., None])
        p_new = jnp.exp(s_new - m_top)
        exp_sum = jnp.sum(p_cache, axis=-1) + p_new
        weighted = jnp.einsum('gqs,sgd->gqd', p_cache, v_row.astype(jnp.float32))
        weighted = weighted + p_new[..., None] * v_tok.astype(jnp.float32)[:, None, :]
        return (weighted / exp_sum[..., None]).reshape(Q_COLS).astype(jnp.bfloat16)

    attn_rows = lax.map(one_row, (q_rot, k_cache, v_cache, k_rot, v_new, seq_lens))
    y_out = (x_f32 + jnp.dot(attn_rows, w_o, preferred_element_type=jnp.float32)).astype(jnp.bfloat16)
    return y_out, k_rot, v_new
```

```python
import functools

import jax
import jax.numpy as jnp
from jax import lax
from jax.experimental import pallas as pl
from jax.experimental.pallas import tpu as pltpu
from jax.sharding import PartitionSpec as P

RMS_EPS = 1.5625e-7
ROPE_BASE = 10000.0
NEG_BIG = -1e30
F32 = jnp.float32
BF16 = jnp.bfloat16
MESH = pl.DeviceIdType.MESH
HALF = 16
ML_ROWS = HALF + 1
VMEM_SPEC = pl.BlockSpec(memory_space=pltpu.VMEM)
ANY_SPEC = pl.BlockSpec(memory_space=pl.ANY)


def rope(heads, cos_t, sin_t):
    lane = lax.broadcasted_iota(jnp.int32, heads.shape, 1)
    width = heads.shape[1]
    swapped = jnp.where(lane % 2 == 0, pltpu.roll(heads, width - 1, 1), pltpu.roll(heads, 1, 1))
    rotated = (heads * cos_t + swapped * sin_t).astype(BF16).astype(F32)
    return jnp.where(lane < width // 2, rotated, heads)


def qkv_kernel(n_tiles, head_dim, hid_ref, nw_ref, cos_ref, sin_ref, wq_ref, bq_ref, wk_ref, bk_ref, wv_ref, bv_ref,
               q_ref, k_ref, v_ref, kb_ref, vb_ref, normed, wk_buf, wv_buf, sems):
    step = pl.program_id(0)
    n_rows = hid_ref.shape[0]

    def small_copies():
        return (pltpu.make_async_copy(wk_ref, wk_buf, sems.at[0]), pltpu.make_async_copy(wv_ref, wv_buf, sems.at[1]))

    @pl.when(step == 0)
    def _():
        for copy in small_copies():
            copy.start()

        def norm_rows(i, carry):
            rows = pl.ds(pl.multiple_of(i * 16, 16), 16)
            x = hid_ref[rows, :].astype(F32)
            mean_sq = jnp.mean(x * x, axis=1, keepdims=True)
            normed[rows, :] = (x * lax.rsqrt(mean_sq + RMS_EPS) * nw_ref[...]).astype(BF16)
            return carry
        lax.fori_loop(0, n_rows // 16, norm_rows, 0)

    @pl.when(step < n_tiles)
    def _():
        acc = jnp.dot(normed[...], wq_ref[...], preferred_element_type=F32) + bq_ref[0]
        acc = acc.astype(BF16).astype(F32)
        for h in range(acc.shape[1] // head_dim):
            q_ref[h * n_rows:(h + 1) * n_rows, :] = rope(acc[:, h * head_dim:(h + 1) * head_dim], cos_ref[...], sin_ref[...])

    @pl.when(step == n_tiles)
    def _():
        for copy in small_copies():
            copy.wait()
        k = (jnp.dot(normed[...], wk_buf[...], preferred_element_type=F32) + bk_ref[...]).astype(BF16).astype(F32)
        v = (jnp.dot(normed[...], wv_buf[...], preferred_element_type=F32) + bv_ref[...]).astype(BF16)
        vb_ref[...] = v
        v = v.astype(F32)
        for g in range(k.shape[1] // head_dim):
            cols = slice(g * head_dim, (g + 1) * head_dim)
            rows = slice(g * n_rows, (g + 1) * n_rows)
            rotated = rope(k[:, cols], cos_ref[...], sin_ref[...])
            k_ref[rows, :] = rotated
            kb_ref[:, cols] = rotated.astype(BF16)
            v_ref[rows, :] = v[:, cols]


def qkv_project(hidden, norm_w, cos_t, sin_t, w_q, b_q, w_k, b_k, w_v, b_v, head_dim):
    n_rows, d_model = hidden.shape
    q_cols, kv_cols = w_q.shape[1], w_k.shape[1]
    tile = 512
    n_tiles = q_cols // tile
    n_heads, n_groups = q_cols // head_dim, kv_cols // head_dim
    last = n_tiles - 1
    whole = lambda shape: pl.BlockSpec(shape, lambda i: (0,) * len(shape))
    return pl.pallas_call(
        functools.partial(qkv_kernel, n_tiles, head_dim),
        grid=(n_tiles + 1,),
        in_specs=[whole((n_rows, d_model)), whole((1, d_model)), whole((n_rows, head_dim)), whole((n_rows, head_dim)),
                  pl.BlockSpec((d_model, tile), lambda i: (0, jnp.minimum(i, last))),
                  pl.BlockSpec((1, 1, tile), lambda i: (jnp.minimum(i, last), 0, 0)),
                  ANY_SPEC, whole((1, kv_cols)), ANY_SPEC, whole((1, kv_cols))],
        out_specs=[pl.BlockSpec((n_rows * tile // head_dim, head_dim), lambda i: (jnp.minimum(i, last), 0)),
                   whole((n_groups * n_rows, head_dim)), whole((n_groups * n_rows, head_dim)),
                   whole((n_rows, kv_cols)), whole((n_rows, kv_cols))],
        out_shape=[jax.ShapeDtypeStruct((n_heads * n_rows, head_dim), F32),
                   jax.ShapeDtypeStruct((n_groups * n_rows, head_dim), F32),
                   jax.ShapeDtypeStruct((n_groups * n_rows, head_dim), F32),
                   jax.ShapeDtypeStruct((n_rows, kv_cols), BF16), jax.ShapeDtypeStruct((n_rows, kv_cols), BF16)],
        scratch_shapes=[pltpu.VMEM((n_rows, d_model), BF16), pltpu.VMEM((d_model, kv_cols), BF16),
                        pltpu.VMEM((d_model, kv_cols), BF16), pltpu.SemaphoreType.DMA((2,))],
        compiler_params=pltpu.CompilerParams(dimension_semantics=("arbitrary",), vmem_limit_bytes=48 * 2 ** 20),
        name="qkv",
    )(hidden, norm_w.astype(F32).reshape(1, d_model), cos_t, sin_t, w_q, b_q.astype(F32).reshape(n_tiles, 1, tile),
      w_k, b_k.astype(F32).reshape(1, kv_cols), w_v, b_v.astype(F32).reshape(1, kv_cols))


def attn_kernel(n_rows, n_heads, n_groups, block_rows, lens_ref, q_ref, kn_ref, vn_ref, k_ref, v_ref, o_ref):
    step = pl.program_id(0)
    shard = lax.axis_index('sp')
    per_row = k_ref.shape[0] // block_rows
    s_dev = per_row // n_groups
    head_dim = k_ref.shape[1]
    scale = head_dim ** -0.5
    unroll = 8
    per_group = n_heads // n_groups
    col = lax.broadcasted_iota(jnp.int32, (n_heads, per_row), 1)
    head = lax.broadcasted_iota(jnp.int32, (n_heads, per_row), 0)
    cache_pos = jnp.where(col % n_groups == head // per_group, col // n_groups + shard * s_dev, jnp.int32(2 ** 30))
    head_d = lax.broadcasted_iota(jnp.int32, (n_heads, head_dim), 0)
    lane_d = lax.broadcasted_iota(jnp.int32, (n_heads, head_dim), 1)
    new_bias = jnp.where(shard == 0, 0.0, NEG_BIG).astype(F32)
    new_gate = jnp.where(shard == 0, 1.0, 0.0).astype(F32)

    def one_row(half, row, ml):
        local = half * HALF + row
        b = step * block_rows + local
        q = q_ref[pl.ds(b, n_heads, stride=n_rows), :]
        k_new = kn_ref[pl.ds(b, 1), :]
        v_new = vn_ref[pl.ds(b, 1), :]
        for g in range(1, n_groups):
            k_new = jnp.where(head_d < g * per_group, k_new, kn_ref[pl.ds(g * n_rows + b, 1), :])
            v_new = jnp.where(head_d < g * per_group, v_new, vn_ref[pl.ds(g * n_rows + b, 1), :])
        cache = pl.ds(pl.multiple_of(local * per_row, per_row), per_row)
        s = lax.dot_general(q.astype(BF16), k_ref[cache, :], (((1,), (1,)), ((), ())), preferred_element_type=F32) * scale
        valid = cache_pos < lens_ref[b]
        s = jnp.where(valid, s, NEG_BIG)
        s_new = jnp.sum(q * k_new, axis=1, keepdims=True) * scale + new_bias
        m = jnp.maximum(jnp.max(s, axis=1, keepdims=True), s_new)
        p = jnp.where(valid, jnp.exp(s - m), 0.0)
        p_new = jnp.exp(s_new - m) * new_gate
        l = jnp.sum(p, axis=1, keepdims=True) + p_new
        o = jnp.dot(p.astype(BF16), v_ref[cache, :], preferred_element_type=F32) + p_new * v_new
        o_ref[half, row] = o
        ml = jnp.where(lane_d == row, m, ml)
        return jnp.where(lane_d == row + head_dim // 2, l, ml)

    def one_half(half, carry):
        def rows(i, ml):
            for j in range(unroll):
                ml = one_row(half, i * unroll + j, ml)
            return ml
        o_ref[half, HALF] = lax.fori_loop(0, HALF // unroll, rows, jnp.zeros((n_heads, head_dim), F32))
        return carry
    lax.fori_loop(0, block_rows // HALF, one_half, 0)


def local_attention(seq_lens, q, k_new, v_new, k_loc, v_loc, n_heads, n_groups):
    n_rows = seq_lens.shape[0]
    head_dim = q.shape[1]
    block_rows = 32
    per_row = k_loc.shape[0] // n_rows
    whole = lambda shape: pl.BlockSpec(shape, lambda i, lens: (0,) * len(shape))
    cache_spec = pl.BlockSpec((block_rows * per_row, head_dim), lambda i, lens: (i, 0))
    n_halves = n_rows // HALF
    return pl.pallas_call(
        functools.partial(attn_kernel, n_rows, n_heads, n_groups, block_rows),
        grid_spec=pltpu.PrefetchScalarGridSpec(
            num_scalar_prefetch=1, grid=(n_rows // block_rows,),
            in_specs=[whole(q.shape), whole(k_new.shape), whole(v_new.shape), cache_spec, cache_spec],
            out_specs=pl.BlockSpec((block_rows // HALF, ML_ROWS, n_heads, head_dim), lambda i, lens: (i, 0, 0, 0))),
        out_shape=jax.ShapeDtypeStruct((n_halves, ML_ROWS, n_heads, head_dim), F32),
        compiler_params=pltpu.CompilerParams(dimension_semantics=("arbitrary",), vmem_limit_bytes=40 * 2 ** 20),
        name="attn",
    )(seq_lens, q, k_new, v_new, k_loc, v_loc)


def combine(dst, terms):
    planes = [t[HALF] for t in terms]
    shape = planes[0].shape
    lane = lax.broadcasted_iota(jnp.int32, shape, 1)
    top = functools.reduce(jnp.maximum, planes)
    factors = [jnp.exp(p - top) for p in planes]
    sums = sum(p * pltpu.roll(f, shape[1] // 2, 1) for p, f in zip(planes, factors))
    for r in range(HALF):
        dst[r] = sum(t[r] * f[:, r:r + 1] for t, f in zip(terms, factors))
    dst[HALF] = jnp.where(lane < shape[1] // 2, top, sums)


def finish_kernel(n_sp, n_tp, o_ref, hid_ref, wo_ref, out_ref, recv1, comb, d2, from_l, from_r, attn, lhs, w_buf, hid_buf,
                  part, yd2, y_l, y_r, y_buf, send1, recv1_sem, send2, recv2, send3, recv3, send4, recv4, send_d, recv_d,
                  load_sem):
    dp, t, s = lax.axis_index('dp'), lax.axis_index('tp'), lax.axis_index('sp')
    nx = n_sp // 2
    x, c = s // 2, s % 2
    peer = 1 - c
    n_heads, head_dim = o_ref.shape[2], o_ref.shape[3]
    blk_rows = 4 * HALF
    tile = part.shape[2]

    def at(ty, sx, core):
        return (dp, lax.rem(ty + n_tp, n_tp), lax.rem(sx + nx, nx) * 2 + core)

    partner = at(t, x, peer)
    right, left = at(t, x + 1, c), at(t, x - 1, c)
    up, down = at(t + 1, x, c), at(t - 1, x, c)

    def remote(src, dst, ssem, rsem, dev):
        copy = pltpu.make_async_remote_copy(src_ref=src, dst_ref=dst, send_sem=ssem, recv_sem=rsem, device_id=dev,
                                            device_id_type=MESH)
        copy.start()
        return copy

    col0 = c * (n_tp * tile)
    loads = []
    for dt in (2, 1, 3, 0):
        cols = pl.ds(pl.multiple_of(col0 + lax.rem(t + dt, n_tp) * tile, tile), tile)
        loads.append(pltpu.make_async_copy(wo_ref.at[:, cols], w_buf.at[dt], load_sem.at[dt]))
    my_cols = pl.ds(pl.multiple_of(col0 + t * tile, tile), tile)
    my_rows = pl.ds(pl.multiple_of(x * blk_rows, blk_rows), blk_rows)
    loads.append(pltpu.make_async_copy(hid_ref.at[my_rows, my_cols], hid_buf, load_sem.at[4]))
    for load in loads:
        load.start()

    barrier = pltpu.get_barrier_semaphore()
    for dev in (partner, right, left, up, down):
        pl.semaphore_signal(barrier, inc=1, device_id=dev, device_id_type=MESH)
    pl.semaphore_wait(barrier, 5)

    def block_of(dx, core):
        return (lax.rem(x + dx, nx) * 2 + core) * 2
    order = (2, 1, 3, 0)
    first = {dx: remote(o_ref.at[pl.ds(block_of(dx, peer), 2)], recv1.at[dx], send1.at[dx], recv1_sem.at[dx], partner)
             for dx in order}

    def join(dx):
        first[dx].wait_recv()
        for h in range(2):
            combine(comb.at[dx, h], [o_ref.at[block_of(dx, c) + h], recv1.at[dx, h]])

    sends = []
    join(2)
    far_r = remote(comb.at[2, 0], d2.at[0], send2.at[0], recv2.at[0], right)
    far_l = remote(comb.at[2, 1], d2.at[1], send2.at[1], recv2.at[1], left)
    join(1)
    near_r1 = remote(comb.at[1, 1], from_l.at[1], send2.at[2], recv2.at[2], right)
    join(3)
    near_l0 = remote(comb.at[3, 0], from_r.at[0], send2.at[3], recv2.at[3], left)
    join(0)
    far_r.wait_recv()
    combine(comb.at[4, 0], [comb.at[1, 0], d2.at[0]])
    near_r0 = remote(comb.at[4, 0], from_l.at[0], send2.at[4], recv2.at[4], right)
    far_l.wait_recv()
    combine(comb.at[4, 1], [comb.at[3, 1], d2.at[1]])
    near_l1 = remote(comb.at[4, 1], from_r.at[1], send2.at[5], recv2.at[5], left)
    sends += list(first.values()) + [far_r, far_l, near_r1, near_l0, near_r0, near_l1]

    for copy in (near_r1, near_l0, near_r0, near_l1):
        copy.wait_recv()
    for h in range(2):
        combine(recv1.at[0, h], [comb.at[0, h], from_l.at[h], from_r.at[h]])
        plane = recv1[0, h, HALF]
        for r in range(HALF):
            total = recv1[0, h, r]
            attn[c, h * HALF + r] = (total / plane[:, head_dim // 2 + r:head_dim // 2 + r + 1]).astype(BF16).astype(F32)
    share = remote(attn.at[c], attn.at[c], send3.at[0], recv3.at[0], partner)
    sends.append(share)
    share.wait_recv()
    flat = 2 * HALF
    for core in range(2):
        for h in range(n_heads):
            lhs[core * flat:(core + 1) * flat, h * head_dim:(h + 1) * head_dim] = attn[core, :, h, :].astype(BF16)

    half_rows = blk_rows // 2
    lo, hi = pl.ds(0, half_rows), pl.ds(half_rows, half_rows)

    def project(i, dt):
        loads[i].wait()
        part[dt] = jnp.dot(lhs[...], w_buf[dt], preferred_element_type=F32)
    project(0, 2)
    yfar_u = remote(part.at[2, lo], yd2.at[0], send3.at[1], recv3.at[1], up)
    yfar_d = remote(part.at[2, hi], yd2.at[1], send3.at[2], recv3.at[2], down)
    project(1, 1)
    ynear_u1 = remote(part.at[1, hi], y_l.at[1], send3.at[3], recv3.at[3], up)
    project(2, 3)
    ynear_d0 = remote(part.at[3, lo], y_r.at[0], send3.at[4], recv3.at[4], down)
    project(3, 0)
    yfar_u.wait_recv()
    part[4, lo] = part[1, lo] + yd2[0]
    ynear_u0 = remote(part.at[4, lo], y_l.at[0], send3.at[5], recv3.at[5], up)
    yfar_d.wait_recv()
    part[4, hi] = part[3, hi] + yd2[1]
    ynear_d1 = remote(part.at[4, hi], y_r.at[1], send3.at[6], recv3.at[6], down)
    sends += [yfar_u, yfar_d, ynear_u1, ynear_d0, ynear_u0, ynear_d1]
    loads[4].wait()
    for h, (from_d, from_u) in enumerate(((ynear_u0, ynear_d0), (ynear_u1, ynear_d1))):
        from_d.wait_recv()
        from_u.wait_recv()
        rows = pl.ds(h * half_rows, half_rows)
        total = part[0, rows] + y_l[h] + y_r[h] + hid_buf[rows, :].astype(F32)
        y_buf[c, t, x, rows] = total.astype(BF16).astype(F32)

    ici, d2d = [0], [0]
    waits_d = []

    def hop(ty, sx, start, rows, dev):
        piece = y_buf.at[c, lax.rem(ty + n_tp, n_tp), lax.rem(sx + nx, nx), pl.ds(start, rows)]
        i = ici[0]
        ici[0] += 1
        copy = remote(piece, piece, send4.at[i], recv4.at[i], dev)
        sends.append(copy)
        return copy

    def to_partner(ty, sx, start, rows):
        piece = y_buf.at[c, lax.rem(ty + n_tp, n_tp), lax.rem(sx + nx, nx), pl.ds(start, rows)]
        i = d2d[0]
        d2d[0] += 1
        copy = remote(piece, piece, send_d.at[i], recv_d.at[i], partner)
        sends.append(copy)
        waits_d.append(copy)

    quarter = half_rows // 2
    plans = (('y', 0), ('x', half_rows))

    def off(axis, d):
        return (d, 0) if axis == 'y' else (0, d)
    devs = {('y', 1): up, ('y', -1): down, ('x', 1): right, ('x', -1): left}
    other = {'y': 'x', 'x': 'y'}

    def start_piece(axis, base, start):
        ty, sx = t + base[0], x + base[1]
        return (hop(ty, sx, start, half_rows, devs[axis, 1]), hop(ty, sx, start, half_rows, devs[axis, -1]))

    def pass_on(axis, base, start, pair):
        far = []
        for way, (copy, lead) in enumerate(zip(pair, (-1, 1))):
            copy.wait_recv()
            d = off(axis, lead)
            far.append(hop(t + base[0] + d[0], x + base[1] + d[1], start + way * quarter, quarter, devs[axis, -lead]))
        return far

    firsts = {}
    for axis, start in plans:
        firsts[axis] = start_piece(axis, (0, 0), start)
    seconds = {}
    for axis, start in plans:
        seconds[axis, 0] = start_piece(other[axis], (0, 0), start)
        to_partner(t, x, start, half_rows)
    fars = {}
    for axis, start in plans:
        fars[axis] = pass_on(axis, (0, 0), start, firsts[axis])
    for axis, start in plans:
        for lead in (-1, 1):
            d = off(axis, lead)
            seconds[axis, lead] = start_piece(other[axis], d, start)
            to_partner(t + d[0], x + d[1], start, half_rows)
    for axis, start in plans:
        for copy in fars[axis]:
            copy.wait_recv()
        d = off(axis, 2)
        seconds[axis, 2] = start_piece(other[axis], d, start)
        to_partner(t + d[0], x + d[1], start, half_rows)
    last = {}
    for lead in (0, -1, 1, 2):
        for axis, start in plans:
            base = off(axis, lead)
            last[axis, lead] = pass_on(other[axis], base, start, seconds[axis, lead])
            for d in (off(other[axis], -1), off(other[axis], 1)):
                to_partner(t + base[0] + d[0], x + base[1] + d[1], start, half_rows)
    for lead in (0, -1, 1, 2):
        for axis, start in plans:
            base, d = off(axis, lead), off(other[axis], 2)
            for copy in last[axis, lead]:
                copy.wait_recv()
            to_partner(t + base[0] + d[0], x + base[1] + d[1], start, half_rows)
    for copy in waits_d:
        copy.wait_recv()

    def write(i, carry):
        core, ty, sx = i // (n_tp * nx), (i // nx) % n_tp, i % nx
        rows = pl.ds(pl.multiple_of(sx * blk_rows, blk_rows), blk_rows)
        cols = pl.ds(pl.multiple_of(core * (n_tp * tile) + ty * tile, tile), tile)
        out_ref[rows, cols] = y_buf[core, ty, sx].astype(BF16)
        return carry
    lax.fori_loop(0, 2 * n_tp * nx, write, 0)
    for copy in sends:
        copy.wait_send()


def finish(o_parts, hidden, w_o, n_sp, n_tp):
    n_rows, d_model = hidden.shape
    n_halves, _, n_heads, head_dim = o_parts.shape
    nx = n_sp // 2
    tile = d_model // (2 * n_tp)
    blk = 4 * HALF
    half_shape = (ML_ROWS, n_heads, head_dim)
    dma = pltpu.SemaphoreType.DMA
    return pl.pallas_call(
        functools.partial(finish_kernel, n_sp, n_tp),
        in_specs=[VMEM_SPEC, ANY_SPEC, ANY_SPEC],
        out_specs=VMEM_SPEC,
        out_shape=jax.ShapeDtypeStruct((n_rows, d_model), BF16),
        scratch_shapes=[
            pltpu.VMEM((nx, 2) + half_shape, F32), pltpu.VMEM((nx + 1, 2) + half_shape, F32),
            pltpu.VMEM((2,) + half_shape, F32), pltpu.VMEM((2,) + half_shape, F32), pltpu.VMEM((2,) + half_shape, F32),
            pltpu.VMEM((2, 2 * HALF, n_heads, head_dim), F32), pltpu.VMEM((blk, n_heads * head_dim), BF16),
            pltpu.VMEM((n_tp, n_heads * head_dim, tile), BF16), pltpu.VMEM((blk, tile), BF16),
            pltpu.VMEM((n_tp + 1, blk, tile), F32), pltpu.VMEM((2, blk // 2, tile), F32),
            pltpu.VMEM((2, blk // 2, tile), F32), pltpu.VMEM((2, blk // 2, tile), F32),
            pltpu.VMEM((2, n_tp, nx, blk, tile), F32),
            dma((4,)), dma((4,)), dma((6,)), dma((6,)), dma((7,)), dma((7,)), dma((40,)), dma((40,)), dma((32,)), dma((32,)),
            dma((5,))],
        compiler_params=pltpu.CompilerParams(collective_id=0, has_side_effects=True, vmem_limit_bytes=60 * 2 ** 20),
        name="finish",
    )(o_parts, hidden, w_o)


def solution(mesh):
    n_sp, n_tp = mesh.shape['sp'], mesh.shape['tp']

    def device_step(hidden, norm_w, w_q, b_q, w_k, b_k, w_v, b_v, w_o, k_cache, v_cache, positions, seq_lens):
        n_rows = hidden.shape[0]
        groups_dev, head_dim = k_cache.shape[2], k_cache.shape[3]
        heads_dev = w_q.shape[1] // head_dim
        rot_dim = head_dim // 2
        lane = jnp.arange(head_dim, dtype=jnp.int32)
        inv_freq = ROPE_BASE ** (-2.0 * (lane // 2).astype(F32) / rot_dim)
        angles = positions.astype(F32)[:, None] * inv_freq
        cos_t = jnp.cos(angles)
        sin_t = jnp.where(lane % 2 == 0, -jnp.sin(angles), jnp.sin(angles))
        q, k_rot, v_row, k_out, v_out = qkv_project(hidden, norm_w, cos_t, sin_t, w_q, b_q, w_k, b_k, w_v, b_v, head_dim)
        o_parts = local_attention(seq_lens, q, k_rot, v_row, k_cache.reshape(-1, head_dim), v_cache.reshape(-1, head_dim),
                                  heads_dev, groups_dev)
        y_out = finish(o_parts, hidden, w_o, n_sp, n_tp)
        return y_out, k_out.reshape(n_rows, groups_dev, head_dim), v_out.reshape(n_rows, groups_dev, head_dim)

    col_spec = P(None, 'tp')
    vec_spec = P('tp')
    cache_spec = P('dp', 'sp', 'tp', None)
    group_spec = P('dp', 'tp', None)
    in_specs = (P('dp', None), P(None), col_spec, vec_spec, col_spec, vec_spec, col_spec, vec_spec,
                P('tp', None), cache_spec, cache_spec, P('dp'), P('dp'))
    out_specs = (P('dp', None), group_spec, group_spec)
    return jax.shard_map(device_step, mesh=mesh, in_specs=in_specs, out_specs=out_specs, check_vma=False)
```

```python
import functools

import jax
import jax.numpy as jnp
from jax import lax
from jax.experimental import pallas as pl
from jax.experimental.pallas import tpu as pltpu
from jax.sharding import PartitionSpec as P

RMS_EPS = 1.5625e-7
ROPE_BASE = 10000.0
NEG_BIG = -1e30
F32 = jnp.float32
BF16 = jnp.bfloat16
MESH = pl.DeviceIdType.MESH
HALF = 16
ML_ROWS = HALF + 1
VMEM_SPEC = pl.BlockSpec(memory_space=pltpu.VMEM)
ANY_SPEC = pl.BlockSpec(memory_space=pl.ANY)


def rope(heads, cos_t, sin_t):
    lane = lax.broadcasted_iota(jnp.int32, heads.shape, 1)
    width = heads.shape[1]
    swapped = jnp.where(lane % 2 == 0, pltpu.roll(heads, width - 1, 1), pltpu.roll(heads, 1, 1))
    rotated = (heads * cos_t + swapped * sin_t).astype(BF16).astype(F32)
    return jnp.where(lane < width // 2, rotated, heads)


def combine(dst, terms):
    planes = [t[HALF] for t in terms]
    shape = planes[0].shape
    lane = lax.broadcasted_iota(jnp.int32, shape, 1)
    top = functools.reduce(jnp.maximum, planes)
    factors = [jnp.exp(p - top) for p in planes]
    sums = sum(p * pltpu.roll(f, shape[1] // 2, 1) for p, f in zip(planes, factors))
    for r in range(HALF):
        dst[r] = sum(t[r] * f[:, r:r + 1] for t, f in zip(terms, factors))
    dst[HALF] = jnp.where(lane < shape[1] // 2, top, sums)


GROUP = 8
SLOTS = 6


def step_kernel(n_sp, n_tp, n_groups, lens_ref, hid_ref, vec_ref, cos_ref, sin_ref, wq_ref, wk_ref, wv_ref, wo_ref, k_ref,
                v_ref, out_ref, kb_ref, vb_ref, hid, w_buf, wk_buf, wv_buf, q_scr, kn, vn, k_buf, v_buf, s_buf, o_scr,
                recv1, comb, d2, from_l, from_r, attn, lhs, hid_buf, part, yd2, y_l, y_r, y_buf, load_sem, kv_sem,
                sendq, recvq, send1, recv1_sem, send2, recv2, send3, recv3, send4, recv4, send_d, recv_d):
    dp, t, s = lax.axis_index('dp'), lax.axis_index('tp'), lax.axis_index('sp')
    nx = n_sp // 2
    x, c = s // 2, s % 2
    peer = 1 - c
    n_rows, d_model = hid.shape
    head_dim = q_scr.shape[1]
    n_heads = q_scr.shape[0] // n_rows
    per_group = n_heads // n_groups
    per_row = k_buf.shape[1] // HALF
    s_dev = per_row // n_groups
    tile = w_buf.shape[1]
    q_tiles = n_heads * head_dim // (2 * tile)
    heads_tile = tile // head_dim
    blk_rows = 4 * HALF
    scale = head_dim ** -0.5

    def at(ty, sx, core):
        return (dp, lax.rem(ty + n_tp, n_tp), lax.rem(sx + nx, nx) * 2 + core)

    partner = at(t, x, peer)
    right, left = at(t, x + 1, c), at(t, x - 1, c)
    up, down = at(t + 1, x, c), at(t - 1, x, c)

    def remote_copy(src, dst, ssem, rsem, dev):
        return pltpu.make_async_remote_copy(src_ref=src, dst_ref=dst, send_sem=ssem, recv_sem=rsem, device_id=dev,
                                            device_id_type=MESH)

    def remote(*args):
        copy = remote_copy(*args)
        copy.start()
        return copy

    load_hid = pltpu.make_async_copy(hid_ref, hid, load_sem.at[0])
    load_q = [pltpu.make_async_copy(wq_ref.at[:, pl.ds(pl.multiple_of((c * q_tiles + i) * tile, tile), tile)],
                                    w_buf.at[pl.ds(i * d_model, d_model)], load_sem.at[1 + i]) for i in range(q_tiles)]
    my_group = pl.ds(pl.multiple_of(c * head_dim, head_dim), head_dim)
    load_k = pltpu.make_async_copy(wk_ref.at[:, my_group], wk_buf, load_sem.at[1 + q_tiles])
    load_v = pltpu.make_async_copy(wv_ref.at[:, my_group], wv_buf, load_sem.at[2 + q_tiles])
    load_hid.start()
    for load in load_q:
        load.start()
    load_k.start()
    load_v.start()
    my_cols = pl.ds(pl.multiple_of((c * n_tp + t) * tile, tile), tile)
    my_rows = pl.ds(pl.multiple_of(x * blk_rows, blk_rows), blk_rows)
    load_res = pltpu.make_async_copy(hid_ref.at[my_rows, my_cols], hid_buf, load_sem.at[3 + q_tiles])
    load_res.start()

    barrier = pltpu.get_barrier_semaphore()
    for dev in (partner, right, left, up, down):
        pl.semaphore_signal(barrier, inc=1, device_id=dev, device_id_type=MESH)

    def half_block(i, j):
        k = i // 2
        side = jnp.where(j == 0, 1, 3)
        dx = jnp.where(k == 0, 2, jnp.where(k == 3, 0, side))
        h = jnp.where(k == 1, 1 - j, j)
        core = jnp.where(i % 2 == 0, peer, c)
        return (lax.rem(x + dx, nx) * 2 + core) * 2 + h

    def cache_copies(i, j):
        slot = lax.rem(i * 2 + j, SLOTS)
        rows = pl.ds(pl.multiple_of(half_block(i, j) * (HALF * per_row), HALF * per_row), HALF * per_row)
        return (pltpu.make_async_copy(k_ref.at[rows], k_buf.at[slot], kv_sem.at[slot * 2]),
                pltpu.make_async_copy(v_ref.at[rows], v_buf.at[slot], kv_sem.at[slot * 2 + 1]))

    def start_cache(i):
        for j in range(2):
            for copy in cache_copies(i, j):
                copy.start()

    def wait_cache(i):
        for j in range(2):
            for copy in cache_copies(i, j):
                copy.wait()

    load_hid.wait()

    def norm_rows(i, carry):
        rows = pl.ds(pl.multiple_of(i * 16, 16), 16)
        xr = hid[rows, :].astype(F32)
        mean_sq = jnp.mean(xr * xr, axis=1, keepdims=True)
        hid[rows, :] = (xr * lax.rsqrt(mean_sq + RMS_EPS) * vec_ref[:, :d_model]).astype(BF16)
        return carry
    lax.fori_loop(0, n_rows // 16, norm_rows, 0)
    for i in range(SLOTS // 2):
        start_cache(i)

    pl.semaphore_wait(barrier, 5)
    shared = []
    for i in range(q_tiles):
        load_q[i].wait()
        first = (c * q_tiles + i) * heads_tile
        bias = vec_ref[:, pl.ds(pl.multiple_of(d_model + first * head_dim, head_dim), tile)]
        acc = jnp.dot(hid[...], w_buf[i * d_model:(i + 1) * d_model, :], preferred_element_type=F32) + bias
        acc = acc.astype(BF16).astype(F32)
        for h in range(heads_tile):
            rows = pl.ds(pl.multiple_of((first + h) * n_rows, n_rows), n_rows)
            q_scr[rows, :] = rope(acc[:, h * head_dim:(h + 1) * head_dim], cos_ref[...], sin_ref[...])
        piece = q_scr.at[pl.ds(pl.multiple_of(first * n_rows, n_rows), heads_tile * n_rows)]
        shared.append(remote(piece, piece, sendq.at[i], recvq.at[i], partner))
    load_k.wait()
    load_v.wait()
    rows = pl.ds(pl.multiple_of(c * n_rows, n_rows), n_rows)
    bias_at = d_model + n_heads * head_dim + c * head_dim
    b_k = vec_ref[:, pl.ds(pl.multiple_of(bias_at, head_dim), head_dim)]
    b_v = vec_ref[:, pl.ds(pl.multiple_of(bias_at + n_groups * head_dim, head_dim), head_dim)]
    k_row = (jnp.dot(hid[...], wk_buf[...], preferred_element_type=F32) + b_k).astype(BF16).astype(F32)
    kn[rows, :] = rope(k_row, cos_ref[...], sin_ref[...])
    shared.append(remote(kn.at[rows], kn.at[rows], sendq.at[q_tiles], recvq.at[q_tiles], partner))
    vn[rows, :] = (jnp.dot(hid[...], wv_buf[...], preferred_element_type=F32) + b_v).astype(BF16).astype(F32)
    shared.append(remote(vn.at[rows], vn.at[rows], sendq.at[q_tiles + 1], recvq.at[q_tiles + 1], partner))
    for copy in shared:
        copy.wait_recv()

    col = lax.broadcasted_iota(jnp.int32, (n_heads, per_row), 1)
    head = lax.broadcasted_iota(jnp.int32, (n_heads, per_row), 0)
    cache_pos = jnp.where(col % n_groups == head // per_group, col // n_groups + s * s_dev, jnp.int32(2 ** 30))
    head_d = lax.broadcasted_iota(jnp.int32, (n_heads, head_dim), 0)
    lane_d = lax.broadcasted_iota(jnp.int32, (n_heads, head_dim), 1)
    new_bias = jnp.where(s == 0, 0.0, NEG_BIG).astype(F32)
    new_gate = jnp.where(s == 0, 1.0, 0.0).astype(F32)

    def scores(i, g):
        j = g * GROUP // HALF
        slot = lax.rem(i * 2 + j, SLOTS)
        b0 = half_block(i, j) * HALF
        for r in range(GROUP):
            row = g * GROUP % HALF + r
            q = q_scr[pl.ds(b0 + row, n_heads, stride=n_rows), :]
            k = k_buf[slot, row * per_row:(row + 1) * per_row, :]
            s_buf[g % 2, r] = lax.dot_general(q.astype(BF16), k, (((1,), (1,)), ((), ())), preferred_element_type=F32)

    def outputs(i, g, ml):
        j = g * GROUP // HALF
        slot = lax.rem(i * 2 + j, SLOTS)
        hb = half_block(i, j)
        probs = []
        for r in range(GROUP):
            row = g * GROUP % HALF + r
            b = hb * HALF + row
            q = q_scr[pl.ds(b, n_heads, stride=n_rows), :]
            k_new, v_new = kn[pl.ds(b, 1), :], vn[pl.ds(b, 1), :]
            for gr in range(1, n_groups):
                k_new = jnp.where(head_d < gr * per_group, k_new, kn[pl.ds(gr * n_rows + b, 1), :])
                v_new = jnp.where(head_d < gr * per_group, v_new, vn[pl.ds(gr * n_rows + b, 1), :])
            valid = cache_pos < lens_ref[b]
            sc = jnp.where(valid, s_buf[g % 2, r] * scale, NEG_BIG)
            s_new = jnp.sum(q * k_new, axis=1, keepdims=True) * scale + new_bias
            m = jnp.maximum(jnp.max(sc, axis=1, keepdims=True), s_new)
            p = jnp.where(valid, jnp.exp(sc - m), 0.0)
            p_new = jnp.exp(s_new - m) * new_gate
            l = jnp.sum(p, axis=1, keepdims=True) + p_new
            ml = jnp.where(lane_d == row, m, ml)
            ml = jnp.where(lane_d == row + head_dim // 2, l, ml)
            probs.append((row, p.astype(BF16), p_new * v_new))
        for row, p, extra in probs:
            v = v_buf[slot, row * per_row:(row + 1) * per_row, :]
            o_scr[hb, row] = jnp.dot(p, v, preferred_element_type=F32) + extra
        return ml

    def load_o(n):
        dt = jnp.where(n == 0, 2, jnp.where(n == 3, 0, jnp.where(n == 1, 1, 3)))
        depth = n_heads * head_dim
        cols = pl.ds(pl.multiple_of((c * n_tp + lax.rem(t + dt, n_tp)) * tile, tile), tile)
        return pltpu.make_async_copy(wo_ref.at[:, cols], w_buf.at[pl.ds(pl.multiple_of(n * depth, depth), depth)],
                                     load_sem.at[n])

    def to_core(k, j):
        return remote_copy(o_scr.at[half_block(2 * k, j)], recv1.at[k, j], send1.at[2 * k + j], recv1_sem.at[2 * k + j],
                           partner)

    far_r = remote_copy(comb.at[0, 0], d2.at[0], send2.at[0], recv2.at[0], right)
    far_l = remote_copy(comb.at[0, 1], d2.at[1], send2.at[1], recv2.at[1], left)
    near_r1 = remote_copy(comb.at[1, 0], from_l.at[1], send2.at[2], recv2.at[2], right)
    near_l0 = remote_copy(comb.at[1, 1], from_r.at[0], send2.at[3], recv2.at[3], left)
    near_r0 = remote_copy(comb.at[2, 0], from_l.at[0], send2.at[4], recv2.at[4], right)
    near_l1 = remote_copy(comb.at[2, 1], from_r.at[1], send2.at[5], recv2.at[5], left)
    n_units = n_rows // (2 * HALF)
    n_groups_unit = 2 * HALF // GROUP

    wait_cache(0)
    scores(0, 0)

    def unit(i, carry):
        nxt = jnp.minimum(i + 1, n_units - 1)

        @pl.when(i < n_units - 1)
        def _():
            wait_cache(i + 1)

        @pl.when(i < n_tp)
        def _():
            load_o(i).start()
        ml = jnp.zeros((n_heads, head_dim), F32)
        for g in range(n_groups_unit):
            if g < n_groups_unit - 1:
                scores(i, g + 1)
            else:
                scores(nxt, 0)
            ml = outputs(i, g, ml)
            if (g + 1) * GROUP % HALF == 0:
                o_scr[half_block(i, g * GROUP // HALF), HALF] = ml
                ml = jnp.zeros((n_heads, head_dim), F32)

        @pl.when(i + SLOTS // 2 < n_units)
        def _():
            start_cache(i + SLOTS // 2)

        k = i // 2

        @pl.when(i % 2 == 0)
        def _():
            for j in range(2):
                to_core(k, j).start()

        @pl.when(i % 2 == 1)
        def _():
            for j in range(2):
                to_core(k, j).wait_recv()

            @pl.when(k < 2)
            def _():
                for j in range(2):
                    combine(comb.at[k, j], [o_scr.at[half_block(i, j)], recv1.at[k, j]])

            @pl.when(k == 0)
            def _():
                far_r.start()
                far_l.start()

            @pl.when(k == 1)
            def _():
                near_r1.start()
                near_l0.start()

            @pl.when(k == 2)
            def _():
                far_r.wait_recv()
                combine(comb.at[2, 0], [o_scr.at[half_block(i, 0)], recv1.at[2, 0], d2.at[0]])
                near_r0.start()
                far_l.wait_recv()
                combine(comb.at[2, 1], [o_scr.at[half_block(i, 1)], recv1.at[2, 1], d2.at[1]])
                near_l1.start()
        return carry
    lax.fori_loop(0, n_units, unit, 0)

    for g in range(n_groups):
        cols = slice(g * head_dim, (g + 1) * head_dim)
        kb_ref[:, cols] = kn[g * n_rows:(g + 1) * n_rows, :].astype(BF16)
        vb_ref[:, cols] = vn[g * n_rows:(g + 1) * n_rows, :].astype(BF16)

    sends = shared + [to_core(k, j) for k in range(4) for j in range(2)]
    sends += [far_r, far_l, near_r1, near_l0, near_r0, near_l1]
    for h, pair in enumerate(((near_l0, near_r0), (near_r1, near_l1))):
        for copy in pair:
            copy.wait_recv()
        own = half_block(n_units - 1, h)
        combine(comb.at[3, h], [o_scr.at[own], recv1.at[3, h], from_l.at[h], from_r.at[h]])
        plane = comb[3, h, HALF]
        for r in range(HALF):
            total = comb[3, h, r]
            attn[c, h * HALF + r] = (total / plane[:, head_dim // 2 + r:head_dim // 2 + r + 1]).astype(BF16).astype(F32)
    share = remote(attn.at[c], attn.at[c], send3.at[0], recv3.at[0], partner)
    sends.append(share)
    share.wait_recv()
    flat = 2 * HALF
    for core in range(2):
        for h in range(n_heads):
            lhs[core * flat:(core + 1) * flat, h * head_dim:(h + 1) * head_dim] = attn[core, :, h, :].astype(BF16)

    half_rows = blk_rows // 2
    lo, hi = pl.ds(0, half_rows), pl.ds(half_rows, half_rows)

    def project(i, dt):
        load_o(i).wait()
        depth = n_heads * head_dim
        part[dt] = jnp.dot(lhs[...], w_buf[i * depth:(i + 1) * depth, :], preferred_element_type=F32)
    project(0, 2)
    yfar_u = remote(part.at[2, lo], yd2.at[0], send3.at[1], recv3.at[1], up)
    yfar_d = remote(part.at[2, hi], yd2.at[1], send3.at[2], recv3.at[2], down)
    project(1, 1)
    ynear_u1 = remote(part.at[1, hi], y_l.at[1], send3.at[3], recv3.at[3], up)
    project(2, 3)
    ynear_d0 = remote(part.at[3, lo], y_r.at[0], send3.at[4], recv3.at[4], down)
    project(3, 0)
    yfar_u.wait_recv()
    part[4, lo] = part[1, lo] + yd2[0]
    ynear_u0 = remote(part.at[4, lo], y_l.at[0], send3.at[5], recv3.at[5], up)
    yfar_d.wait_recv()
    part[4, hi] = part[3, hi] + yd2[1]
    ynear_d1 = remote(part.at[4, hi], y_r.at[1], send3.at[6], recv3.at[6], down)
    sends += [yfar_u, yfar_d, ynear_u1, ynear_d0, ynear_u0, ynear_d1]
    load_res.wait()
    for h, (from_d, from_u) in enumerate(((ynear_u0, ynear_d0), (ynear_u1, ynear_d1))):
        from_d.wait_recv()
        from_u.wait_recv()
        rows = pl.ds(h * half_rows, half_rows)
        total = part[0, rows] + y_l[h] + y_r[h] + hid_buf[rows, :].astype(F32)
        y_buf[c, t, x, rows] = total.astype(BF16).astype(F32)

    ici, d2d = [0], [0]
    waits_d = []

    def hop(ty, sx, start, rows, dev):
        piece = y_buf.at[c, lax.rem(ty + n_tp, n_tp), lax.rem(sx + nx, nx), pl.ds(start, rows)]
        i = ici[0]
        ici[0] += 1
        copy = remote(piece, piece, send4.at[i], recv4.at[i], dev)
        sends.append(copy)
        return copy

    def to_partner(ty, sx, start, rows):
        piece = y_buf.at[c, lax.rem(ty + n_tp, n_tp), lax.rem(sx + nx, nx), pl.ds(start, rows)]
        i = d2d[0]
        d2d[0] += 1
        copy = remote(piece, piece, send_d.at[i], recv_d.at[i], partner)
        sends.append(copy)
        waits_d.append(copy)

    quarter = half_rows // 2
    plans = (('y', 0), ('x', half_rows))

    def off(axis, d):
        return (d, 0) if axis == 'y' else (0, d)
    devs = {('y', 1): up, ('y', -1): down, ('x', 1): right, ('x', -1): left}
    other = {'y': 'x', 'x': 'y'}

    def start_piece(axis, base, start):
        ty, sx = t + base[0], x + base[1]
        return (hop(ty, sx, start, half_rows, devs[axis, 1]), hop(ty, sx, start, half_rows, devs[axis, -1]))

    def pass_on(axis, base, start, pair):
        far = []
        for way, (copy, lead) in enumerate(zip(pair, (-1, 1))):
            copy.wait_recv()
            d = off(axis, lead)
            far.append(hop(t + base[0] + d[0], x + base[1] + d[1], start + way * quarter, quarter, devs[axis, -lead]))
        return far

    firsts = {}
    for axis, start in plans:
        firsts[axis] = start_piece(axis, (0, 0), start)
    seconds = {}
    for axis, start in plans:
        seconds[axis, 0] = start_piece(other[axis], (0, 0), start)
        to_partner(t, x, start, half_rows)
    fars = {}
    for axis, start in plans:
        fars[axis] = pass_on(axis, (0, 0), start, firsts[axis])
    for axis, start in plans:
        for lead in (-1, 1):
            d = off(axis, lead)
            seconds[axis, lead] = start_piece(other[axis], d, start)
            to_partner(t + d[0], x + d[1], start, half_rows)
    for axis, start in plans:
        for copy in fars[axis]:
            copy.wait_recv()
        d = off(axis, 2)
        seconds[axis, 2] = start_piece(other[axis], d, start)
        to_partner(t + d[0], x + d[1], start, half_rows)
    last = {}
    for lead in (0, -1, 1, 2):
        for axis, start in plans:
            base = off(axis, lead)
            last[axis, lead] = pass_on(other[axis], base, start, seconds[axis, lead])
            for d in (off(other[axis], -1), off(other[axis], 1)):
                to_partner(t + base[0] + d[0], x + base[1] + d[1], start, half_rows)
    for lead in (0, -1, 1, 2):
        for axis, start in plans:
            base, d = off(axis, lead), off(other[axis], 2)
            for copy in last[axis, lead]:
                copy.wait_recv()
            to_partner(t + base[0] + d[0], x + base[1] + d[1], start, half_rows)
    for copy in waits_d:
        copy.wait_recv()

    def write(i, carry):
        core, ty, sx = i // (n_tp * nx), (i // nx) % n_tp, i % nx
        rows = pl.ds(pl.multiple_of(sx * blk_rows, blk_rows), blk_rows)
        cols = pl.ds(pl.multiple_of(core * (n_tp * tile) + ty * tile, tile), tile)
        out_ref[rows, cols] = y_buf[core, ty, sx].astype(BF16)
        return carry
    lax.fori_loop(0, 2 * n_tp * nx, write, 0)
    for copy in sends:
        copy.wait_send()


def attention_step(seq_lens, hidden, vec, cos_t, sin_t, w_q, w_k, w_v, w_o, k_loc, v_loc, n_sp, n_tp, head_dim):
    n_rows, d_model = hidden.shape
    n_heads, n_groups = w_q.shape[1] // head_dim, w_k.shape[1] // head_dim
    nx = n_sp // 2
    tile = d_model // (2 * n_tp)
    blk = 4 * HALF
    per_row = k_loc.shape[0] // n_rows
    half_shape = (ML_ROWS, n_heads, head_dim)
    q_tiles = n_heads * head_dim // (2 * tile)
    dma = pltpu.SemaphoreType.DMA
    kv_out = jax.ShapeDtypeStruct((n_rows, n_groups * head_dim), BF16)
    return pl.pallas_call(
        functools.partial(step_kernel, n_sp, n_tp, n_groups),
        in_specs=[pl.BlockSpec(memory_space=pltpu.SMEM), ANY_SPEC, VMEM_SPEC, VMEM_SPEC, VMEM_SPEC] + [ANY_SPEC] * 6,
        out_specs=[VMEM_SPEC] * 3,
        out_shape=[jax.ShapeDtypeStruct((n_rows, d_model), BF16), kv_out, kv_out],
        scratch_shapes=[
            pltpu.VMEM((n_rows, d_model), BF16), pltpu.VMEM((q_tiles * d_model, tile), BF16),
            pltpu.VMEM((d_model, head_dim), BF16), pltpu.VMEM((d_model, head_dim), BF16),
            pltpu.VMEM((n_heads * n_rows, head_dim), F32), pltpu.VMEM((n_groups * n_rows, head_dim), F32),
            pltpu.VMEM((n_groups * n_rows, head_dim), F32),
            pltpu.VMEM((SLOTS, HALF * per_row, head_dim), BF16), pltpu.VMEM((SLOTS, HALF * per_row, head_dim), BF16),
            pltpu.VMEM((2, GROUP, n_heads, per_row), F32), pltpu.VMEM((n_rows // HALF,) + half_shape, F32),
            pltpu.VMEM((nx, 2) + half_shape, F32), pltpu.VMEM((nx, 2) + half_shape, F32),
            pltpu.VMEM((2,) + half_shape, F32), pltpu.VMEM((2,) + half_shape, F32), pltpu.VMEM((2,) + half_shape, F32),
            pltpu.VMEM((2, 2 * HALF, n_heads, head_dim), F32), pltpu.VMEM((blk, n_heads * head_dim), BF16),
            pltpu.VMEM((blk, tile), BF16), pltpu.VMEM((n_tp + 1, blk, tile), F32), pltpu.VMEM((2, blk // 2, tile), F32),
            pltpu.VMEM((2, blk // 2, tile), F32), pltpu.VMEM((2, blk // 2, tile), F32),
            pltpu.VMEM((2, n_tp, nx, blk, tile), F32),
            dma((q_tiles + 4,)), dma((2 * SLOTS,)), dma((q_tiles + 2,)), dma((q_tiles + 2,)), dma((8,)), dma((8,)),
            dma((6,)), dma((6,)), dma((7,)), dma((7,)), dma((40,)), dma((40,)), dma((32,)), dma((32,))],
        compiler_params=pltpu.CompilerParams(collective_id=0, has_side_effects=True, vmem_limit_bytes=54 * 2 ** 20),
        name="step",
    )(seq_lens, hidden, vec, cos_t, sin_t, w_q, w_k, w_v, w_o, k_loc, v_loc)


def solution(mesh):
    n_sp, n_tp = mesh.shape['sp'], mesh.shape['tp']

    def device_step(hidden, norm_w, w_q, b_q, w_k, b_k, w_v, b_v, w_o, k_cache, v_cache, positions, seq_lens):
        n_rows = hidden.shape[0]
        groups_dev, head_dim = k_cache.shape[2], k_cache.shape[3]
        rot_dim = head_dim // 2
        lane = jnp.arange(head_dim, dtype=jnp.int32)
        inv_freq = ROPE_BASE ** (-2.0 * (lane // 2).astype(F32) / rot_dim)
        angles = positions.astype(F32)[:, None] * inv_freq
        cos_t = jnp.cos(angles)
        sin_t = jnp.where(lane % 2 == 0, -jnp.sin(angles), jnp.sin(angles))
        vec = jnp.concatenate([norm_w, b_q, b_k, b_v]).astype(F32).reshape(1, -1)
        y_out, k_out, v_out = attention_step(seq_lens, hidden, vec, cos_t, sin_t, w_q, w_k, w_v, w_o,
                                             k_cache.reshape(-1, head_dim), v_cache.reshape(-1, head_dim), n_sp, n_tp, head_dim)
        return y_out, k_out.reshape(n_rows, groups_dev, head_dim), v_out.reshape(n_rows, groups_dev, head_dim)

    col_spec = P(None, 'tp')
    vec_spec = P('tp')
    cache_spec = P('dp', 'sp', 'tp', None)
    group_spec = P('dp', 'tp', None)
    in_specs = (P('dp', None), P(None), col_spec, vec_spec, col_spec, vec_spec, col_spec, vec_spec,
                P('tp', None), cache_spec, cache_spec, P('dp'), P('dp'))
    out_specs = (P('dp', None), group_spec, group_spec)
    return jax.shard_map(device_step, mesh=mesh, in_specs=in_specs, out_specs=out_specs, check_vma=False)
```
